32 devices in a mesh: row: 4 (over y, x), col: 8 (over z, core).
Axes of the slice: x: 2, y: 2, z: 4, core: 2. Of those that a mesh axis runs over, the one named last changes fastest.
Arguments:
- features: bfloat16 [8192, 512], P(('row', 'col')), may hold values from -40 to 40
- w_query: bfloat16 [512, 512], replicated, may hold values from -0.25 to 0.25
- w_key: bfloat16 [512, 512], replicated, may hold values from -0.25 to 0.25
- w_value: bfloat16 [512, 512], replicated, may hold values from -0.25 to 0.25
- w_out: bfloat16 [512, 512], replicated, may hold values from -0.25 to 0.25
- pairs: int32 [4, 8, 128, 2], P('row', 'col'), may hold values from 0 to 15, as said below
- counts: int32 [4, 8], P('row', 'col'), may hold values from 16 to 128, as said below
- masks: int32 [4, 8, 128, 128, 4], P('row', 'col'), may hold values from -2147483648 to 2147483646, as said below
Outputs:
- updated: bfloat16 [8192, 512], P(('row', 'col'))
The draws below stay inside these ranges and needn't reach their ends.
Inputs may be any that keep to these rules, and one draw needn't show every extreme that they name: Within one device's list all 128 entries are distinct pairs; the first column is a query tile below 16, the second a key tile below 8. `counts`: some device has a full list of 128 entries in every draw. `masks`: any 32-bit pattern.
All inputs are finite; a program needn't handle non-finite values.
Results may differ from the reference program's by a relative error of at most 0.012.
The reference program's roundings to bfloat16 on the way count: a program that leaves them out, or rounds other values in their place, can miss the bound.
Values may be sent and summed in bfloat16 or wider, within the bound.
No kernel may reach another device: no remote copies, remote signals or barrier semaphores. Data moves between devices by JAX's collectives and lax.ppermute only.
A program may use at most 128 MiB of HBM per device.

```python
import math
import jax
import jax.numpy as jnp
from jax import lax

D = 512
HEADS = 8
HEAD_DIM = 64
TILE = 128
MAXB = 128
NODE_DEV = 256
NODES = 8192
QTILES = 16
KTILES = 8
N_ROW = 4
N_COL = 8


def draw_features(key, part):
    base = jax.random.normal(key, (NODES, D), jnp.float32)
    return jnp.clip(base, -4.0, 4.0).astype(jnp.bfloat16)


def draw_pairs(key, part):
    keys = jax.random.split(jax.random.fold_in(key, 11), N_ROW * N_COL)
    ident = jax.vmap(lambda single: jax.random.permutation(single, QTILES * KTILES)[:MAXB])(keys)
    table = jnp.stack([ident // KTILES, ident % KTILES], -1).astype(jnp.int32)
    return table.reshape(N_ROW, N_COL, MAXB, 2)


def draw_counts(key, part):
    first = jax.random.randint(jax.random.fold_in(key, 1), (N_ROW * N_COL,), 0, MAXB)
    second = jax.random.randint(jax.random.fold_in(key, 2), (N_ROW * N_COL,), 0, MAXB)
    lowest = max(1, MAXB // 8)
    values = jnp.maximum(jnp.minimum(first, second) + 1, lowest)
    chosen = jax.random.randint(jax.random.fold_in(key, 3), (), 0, N_ROW * N_COL)
    values = jnp.where(jnp.arange(N_ROW * N_COL, dtype=jnp.int32) == chosen, MAXB, values)
    return values.astype(jnp.int32).reshape(N_ROW, N_COL)


def draw_masks(key, part):
    shape = (N_ROW, N_COL, MAXB, TILE, TILE // 32)
    return jax.random.randint(jax.random.fold_in(key, 5), shape, -2147483648, 2147483647, jnp.int32)


def noise(stream_key, extent, spread, bound, kind=jnp.bfloat16):
    return jnp.clip(spread * jax.random.normal(stream_key, extent, jnp.float32), -bound, bound).astype(kind)


def setup_inputs(seed: int = 0) -> dict:
    seeds = jax.random.split(jax.random.key(seed), 9)
    features = draw_features(jax.random.fold_in(seeds[8], 71), 0)
    w_query = noise(seeds[1], (D, D), D ** -0.5, 0.25)
    w_key = noise(seeds[2], (D, D), D ** -0.5, 0.25)
    w_value = noise(seeds[3], (D, D), D ** -0.5, 0.25)
    w_out = noise(seeds[4], (D, D), D ** -0.5, 0.25)
    pairs = draw_pairs(jax.random.fold_in(seeds[8], 71), 0)
    counts = draw_counts(jax.random.fold_in(seeds[8], 71), 0)
    masks = draw_masks(jax.random.fold_in(seeds[8], 71), 0)
    return dict(features=features, w_query=w_query, w_key=w_key, w_value=w_value, w_out=w_out, pairs=pairs, counts=counts, masks=masks)


def unpack_bits(words):
    shifts = jnp.broadcast_to(jnp.arange(32, dtype=jnp.int32), words.shape + (32,))
    bits = lax.shift_right_logical(words[..., None], shifts) & 1
    return bits.reshape(words.shape[:-1] + (words.shape[-1] * 32,)) == 1

def device_partial(q_part, k_part, v_part, my_pairs, my_count, my_words):
    scale = 1.0 / math.sqrt(HEAD_DIM)
    tiles_q = q_part.reshape(QTILES, TILE, HEADS, HEAD_DIM)
    tiles_k = k_part.reshape(KTILES, TILE, HEADS, HEAD_DIM)
    tiles_v = v_part.reshape(KTILES, TILE, HEADS, HEAD_DIM)
    qsel = my_pairs[:, 0]
    ksel = my_pairs[:, 1]
    q_blk = tiles_q[qsel].astype(jnp.float32)
    k_blk = tiles_k[ksel].astype(jnp.float32)
    v_blk = tiles_v[ksel].astype(jnp.float32)
    scores = jnp.einsum('gihd,gjhd->ghij', q_blk, k_blk) * scale
    valid = jnp.arange(MAXB, dtype=jnp.int32) < my_count
    live = unpack_bits(my_words) & valid[:, None, None]
    masked = jnp.where(live[:, None], scores, -jnp.inf)
    rowmax = masked.max(-1)
    tmax = jnp.zeros((QTILES, HEADS, TILE), jnp.float32).at[qsel].max(rowmax)
    prob = jnp.where(live[:, None], jnp.exp(scores - tmax[qsel][..., None]), 0.0).astype(jnp.bfloat16)
    probf = prob.astype(jnp.float32)
    den = jnp.exp(-tmax).at[qsel].add(probf.sum(-1))
    weighted = jnp.einsum('ghij,gjhd->gihd', probf, v_blk)
    num = jnp.zeros((QTILES, TILE, HEADS, HEAD_DIM), jnp.float32).at[qsel].add(weighted)
    return (tmax, num, den)

def reference(features, w_query, w_key, w_value, w_out, pairs, counts, masks):
    queries = jnp.dot(features, w_query, preferred_element_type=jnp.float32).astype(jnp.bfloat16)
    keys = jnp.dot(features, w_key, preferred_element_type=jnp.float32).astype(jnp.bfloat16)
    values = jnp.dot(features, w_value, preferred_element_type=jnp.float32).astype(jnp.bfloat16)
    q_rows = NODE_DEV * N_COL
    k_rows = NODE_DEV * N_ROW
    keys_grid = keys.reshape(N_ROW, N_COL, NODE_DEV, D)
    values_grid = values.reshape(N_ROW, N_COL, NODE_DEV, D)

    def per_row(r):
        q_part = lax.dynamic_slice_in_dim(queries, (r * q_rows).astype(jnp.int32), q_rows, 0)

        def per_col(c):
            k_part = lax.dynamic_index_in_dim(keys_grid, c, 1, keepdims=False).reshape(k_rows, D)
            v_part = lax.dynamic_index_in_dim(values_grid, c, 1, keepdims=False).reshape(k_rows, D)
            tmax, num, den = device_partial(q_part, k_part, v_part, pairs[r, c], counts[r, c], masks[r, c])
            part = (num / den.transpose(0, 2, 1)[..., None]).astype(jnp.bfloat16).astype(jnp.float32)
            return (tmax, part, den)
        tmax, part, den = lax.map(per_col, jnp.arange(N_COL, dtype=jnp.int32))
        top = tmax.max(0)
        weight = jnp.exp(tmax - top) * den
        total = weight.sum(0)
        numer = (part * weight.transpose(0, 1, 3, 2)[..., None]).sum(0)
        attended = (numer / total.transpose(0, 2, 1)[..., None]).astype(jnp.bfloat16).reshape(q_rows, D)
        return jnp.dot(attended, w_out, preferred_element_type=jnp.float32).astype(jnp.bfloat16)
    result = lax.map(per_row, jnp.arange(N_ROW, dtype=jnp.int32))
    return result.reshape(NODES, D)
```

```python
import functools
import math

import jax
import jax.numpy as jnp
from jax import lax
from jax.experimental import pallas as pl
from jax.experimental.pallas import tpu as pltpu
from jax.sharding import PartitionSpec as P

HEADS = 8
TILE = 128
GROUP = 4
VMEM = pltpu.VMEM
SMEM = pltpu.SMEM
BF16 = jnp.bfloat16
F32 = jnp.float32
LOG2E = math.log2(math.e)


def vmem():
    return pl.BlockSpec(memory_space=VMEM)


def smem():
    return pl.BlockSpec(memory_space=SMEM)


def exchange(x, axis, bits):
    size = lax.axis_size(axis)
    return lax.ppermute(x, axis, [(i, i ^ bits) for i in range(size)])


def place_kernel(where_ref, pairs_ref, count_ref, words_ref, out_ref, *, qtiles, ktiles):
    row, col = where_ref[0], where_ref[1]
    out_ref[...] = jnp.zeros_like(out_ref)

    def entry(e, carry):
        a, b = pairs_ref[0, e], pairs_ref[1, e]
        chunk = (a // 2) ^ col
        other = chunk % 2
        tile = ((b // 2) ^ row) * 2 + b % 2
        spot = ((other * (qtiles // 4) + chunk // 2) * 2 + a % 2) * ktiles + tile
        out_ref[spot] = words_ref[e]
        return carry

    lax.fori_loop(0, count_ref[0], entry, 0)


def place_masks(pairs, count, words, row, col, qtiles, ktiles):
    return pl.pallas_call(
        functools.partial(place_kernel, qtiles=qtiles, ktiles=ktiles),
        out_shape=jax.ShapeDtypeStruct((qtiles * ktiles, 4, TILE), jnp.int32),
        in_specs=[smem(), smem(), smem(), vmem()],
        out_specs=vmem(),
        name="place",
    )(jnp.stack([row, col]).astype(jnp.int32), pairs.T, count.reshape(1), words)


def nt_dot(a, b):
    return lax.dot_general(a, b, (((1,), (1,)), ((), ())), preferred_element_type=F32)


def project_kernel(f_ref, wk_ref, wvt_ref, k_ref, vt_ref):
    for t in range(f_ref.shape[0] // TILE):
        x = f_ref[t * TILE : (t + 1) * TILE, :]
        k_ref[t] = jnp.dot(x, wk_ref[...], preferred_element_type=F32).astype(BF16)
        vt_ref[t] = nt_dot(wvt_ref[...], x).astype(BF16)


def project(feats, w_key, w_value_t):
    rows, width = feats.shape
    tiles = rows // TILE
    step = 4
    return pl.pallas_call(
        project_kernel,
        grid=(tiles // step,),
        out_shape=(
            jax.ShapeDtypeStruct((tiles, TILE, width), BF16),
            jax.ShapeDtypeStruct((tiles, width, TILE), BF16),
        ),
        in_specs=[
            pl.BlockSpec((step * TILE, width), lambda i: (i, 0)),
            pl.BlockSpec((width, width), lambda i: (0, 0)),
            pl.BlockSpec((width, width), lambda i: (0, 0)),
        ],
        out_specs=(
            pl.BlockSpec((step, TILE, width), lambda i: (i, 0, 0)),
            pl.BlockSpec((step, width, TILE), lambda i: (i, 0, 0)),
        ),
        name="project",
    )(feats, w_key, w_value_t)


def split3(x):
    hi = x.astype(BF16)
    rest = x - hi.astype(F32)
    mid = rest.astype(BF16)
    low = (rest - mid.astype(F32)).astype(BF16)
    return [hi, mid, low]


def attend_kernel(
    used_ref, words_ref, f_ref, wqt_ref, k_ref, vt_ref, out_ref, q_ref, bias_ref, acc_ref, max_ref,
    list_ref, *, sinks
):
    tiles = k_ref.shape[0]
    width = k_ref.shape[2]
    nodes = f_ref.shape[0]
    size = width // HEADS
    factor = LOG2E / math.sqrt(size)

    def gather(n, found):
        list_ref[found] = n
        return found + jnp.where(used_ref[n] != 0, 1, 0)

    found = lax.fori_loop(0, tiles, gather, 0)
    q = nt_dot(wqt_ref[...], f_ref[...]).astype(BF16)
    lower = lax.broadcasted_iota(jnp.int32, (2 * size, nodes), 0) < size
    for h in range(HEADS):
        pair = q[(h // 2) * 2 * size : (h // 2 + 1) * 2 * size, :]
        q_ref[h] = jnp.where(lower == (h % 2 == 0), pair, jnp.zeros_like(pair))
    first = lax.broadcasted_iota(jnp.int32, (size + 16, nodes), 0) == size
    for h in range(HEADS):
        acc_ref[h] = jnp.where(first, F32(sinks), F32(0))
    max_ref[...] = jnp.zeros_like(max_ref)
    bit = lax.shift_left(jnp.int32(1), lax.broadcasted_iota(jnp.int32, (32, TILE), 0))
    ones = jnp.ones((16, TILE * GROUP), BF16)

    def step(i, carry):
        picked = []
        for g in range(GROUP):
            at = i * GROUP + g
            n = list_ref[jnp.minimum(at, found - 1)]
            picked.append(n)
            for t in range(nodes // TILE):
                words = jnp.where(at < found, words_ref[t, n], 0)
                for w in range(4):
                    row = jnp.broadcast_to(words[w : w + 1, :], (32, TILE))
                    bias_ref[g * TILE + w * 32 : g * TILE + w * 32 + 32, t * TILE : (t + 1) * TILE] = (
                        jnp.where((row & bit) != 0, F32(0), F32(-jnp.inf))
                    )
        for h in range(HEADS):
            lanes = slice((h // 2) * 2 * size, (h // 2 + 1) * 2 * size)
            keys = jnp.concatenate([k_ref[n, :, lanes] for n in picked], axis=0)
            s = jnp.dot(keys, q_ref[h], preferred_element_type=F32) + bias_ref[...]
            old = max_ref[h]
            new = jnp.maximum(old, s.max(0, keepdims=True) * factor)
            max_ref[h] = new
            p = jnp.exp2(s * factor - new).astype(BF16)
            values = jnp.concatenate([vt_ref[n, h * size : (h + 1) * size, :] for n in picked], axis=1)
            values = jnp.concatenate([values, ones], axis=0)
            acc_ref[h] = acc_ref[h] * jnp.exp2(old - new) + jnp.dot(
                values, p, preferred_element_type=F32
            )
        return carry

    lax.fori_loop(0, (found + GROUP - 1) // GROUP, step, 0)
    tops, dens = [], []
    for h in range(HEADS):
        den = acc_ref[h, size : size + 1, :]
        out_ref[h * size : (h + 1) * size, :] = (acc_ref[h, 0:size, :] / den).astype(BF16)
        tops.append(max_ref[h])
        dens.append(den)
    stats = split3(jnp.concatenate(tops + dens, axis=0))
    for i, part in enumerate(stats):
        out_ref[width + i * 16 : width + (i + 1) * 16, :] = part


def attend(used, words, feats, w_query_t, keys, values_t, sinks):
    nodes, width = feats.shape
    size = width // HEADS
    return pl.pallas_call(
        functools.partial(attend_kernel, sinks=sinks),
        out_shape=jax.ShapeDtypeStruct((width + 48, nodes), BF16),
        in_specs=[smem(), vmem(), vmem(), vmem(), vmem(), vmem()],
        out_specs=vmem(),
        scratch_shapes=[
            VMEM((HEADS, 2 * size, nodes), BF16),
            VMEM((GROUP * TILE, nodes), F32),
            VMEM((HEADS, size + 16, nodes), F32),
            VMEM((HEADS, 1, nodes), F32),
            SMEM((keys.shape[0] + 1,), jnp.int32),
        ],
        name="attend",
    )(used, words, feats, w_query_t, keys, values_t)


def finish_kernel(*refs):
    parts, (w_ref, out_ref) = refs[:-2], refs[-2:]
    width = w_ref.shape[0]
    size = width // HEADS
    tops, dens = [], []
    for part in parts:
        stats = (
            part[width : width + 16, :].astype(F32)
            + part[width + 16 : width + 32, :].astype(F32)
            + part[width + 32 : width + 48, :].astype(F32)
        )
        tops.append(stats[0:HEADS])
        dens.append(stats[HEADS : 2 * HEADS])
    top = functools.reduce(jnp.maximum, tops)
    weights = [jnp.exp2(t - top) * d for t, d in zip(tops, dens)]
    total = functools.reduce(jnp.add, weights)
    rows = []
    for h in range(HEADS):
        num = functools.reduce(
            jnp.add,
            [
                part[h * size : (h + 1) * size, :].astype(F32) * weight[h : h + 1, :]
                for part, weight in zip(parts, weights)
            ],
        )
        rows.append((num / total[h : h + 1, :]).astype(BF16))
    attended = jnp.concatenate(rows, axis=0)
    out_ref[...] = lax.dot_general(
        attended, w_ref[...], (((0,), (0,)), ((), ())), preferred_element_type=F32
    ).astype(BF16)


def finish(parts, w_out):
    nodes = parts[0].shape[1]
    return pl.pallas_call(
        finish_kernel,
        out_shape=jax.ShapeDtypeStruct((nodes, w_out.shape[1]), BF16),
        in_specs=[vmem()] * (len(parts) + 1),
        out_specs=vmem(),
        name="finish",
    )(*parts, w_out)


def body(features, w_query, w_key, w_value, w_out, pairs, counts, masks):
    nrow, ncol = lax.axis_size("row"), lax.axis_size("col")
    nodes, width = features.shape
    per = nodes // TILE
    qtiles, ktiles = ncol * per, nrow * per
    row, col = lax.axis_index("row"), lax.axis_index("col")
    chips = ncol // 2

    near = [features] + [exchange(features, "row", s) for s in range(1, nrow)]
    asking = [features] + [exchange(features, "col", 2 * s) for s in range(1, chips)]

    words = jnp.swapaxes(masks[0, 0], 1, 2)
    placed = place_masks(pairs[0, 0], counts[0, 0], words, row, col, qtiles, ktiles)
    placed = placed.reshape(2, chips, per, ktiles, 4, TILE)
    words = jnp.concatenate([placed[0], exchange(placed[1], "col", 1)], axis=2)
    used = (words != 0).any((1, 3, 4)).astype(jnp.int32)

    mine = jnp.concatenate(near, axis=0)
    feats = jnp.concatenate([mine, exchange(mine, "col", 1)], axis=0)
    keys, values_t = project(feats, w_key, w_value.T)
    w_query_t = w_query.T

    parts = [None] * chips
    for s in list(range(1, chips)) + [0]:
        part = attend(used[s], words[s], asking[s], w_query_t, keys, values_t, 2)
        parts[s] = part if s == 0 else exchange(part, "col", 2 * s)
    return finish(parts, w_out)


def solution(mesh):
    in_specs = (
        P(("row", "col"), None),
        P(),
        P(),
        P(),
        P(),
        P("row", "col", None, None),
        P("row", "col"),
        P("row", "col", None, None, None),
    )
    out_specs = P(("row", "col"), None)
    return jax.shard_map(body, mesh=mesh, in_specs=in_specs, out_specs=out_specs, check_vma=False)
```

```python
import functools
import math

import jax
import jax.numpy as jnp
from jax import lax
from jax.experimental import pallas as pl
from jax.experimental.pallas import tpu as pltpu
from jax.sharding import PartitionSpec as P


HEADS = 8
TILE = 128
GROUP = 4
LIMIT = 24 * 1024 * 1024
VMEM = pltpu.VMEM
SMEM = pltpu.SMEM
BF16 = jnp.bfloat16
F32 = jnp.float32
LOG2E = math.log2(math.e)


def vmem():
    return pl.BlockSpec(memory_space=VMEM)


def smem():
    return pl.BlockSpec(memory_space=SMEM)


def exchange(x, axis, bits):
    size = lax.axis_size(axis)
    return lax.ppermute(x, axis, [(i, i ^ bits) for i in range(size)])


def index_kernel(where_ref, mine_ref, other_ref, out_ref, *, tiles, entries):
    row, col = where_ref[0], where_ref[1]

    def clear(i, carry):
        out_ref[i] = -1
        return carry

    lax.fori_loop(0, out_ref.shape[0], clear, 0)
    for side, ref in enumerate((mine_ref, other_ref)):

        def entry(e, carry, side=side, ref=ref):
            a, b = ref[2 * e], ref[2 * e + 1]
            chunk = (a // 2) ^ col
            tile = ((b // 2) ^ row) * 4 + side * 2 + b % 2

            @pl.when(chunk % 2 == 0)
            def _():
                out_ref[(chunk + a % 2) * tiles + tile] = e

            return carry

        lax.fori_loop(0, ref[2 * entries], entry, 0)


def index(mine, other, row, col, size, tiles, entries):
    return pl.pallas_call(
        functools.partial(index_kernel, tiles=tiles, entries=entries),
        out_shape=jax.ShapeDtypeStruct((size,), jnp.int32),
        in_specs=[smem(), smem(), smem()],
        out_specs=smem(),
        name="index",
    )(jnp.stack([row, col]).astype(jnp.int32), mine, other)


def nt_dot(a, b):
    return lax.dot_general(a, b, (((1,), (1,)), ((), ())), preferred_element_type=F32)


def project_kernel(mine_ref, other_ref, wk_ref, wvt_ref, *refs):
    k_ref, vt_ref, norm_ref = refs[-3:]
    double = k_ref.shape[3]
    width = wk_ref.shape[0]
    lane = lax.broadcasted_iota(jnp.int32, (width, TILE), 1)
    head = lax.broadcasted_iota(jnp.int32, (width, TILE), 0) // (double // 2)
    pick = jnp.where(lane == head, F32(1.01), F32(0)).astype(BF16)
    x = jnp.concatenate([mine_ref[...], other_ref[...]], axis=0)
    rows = x.shape[0]
    k = jnp.dot(x, wk_ref[...], preferred_element_type=F32).astype(BF16)
    v = nt_dot(wvt_ref[...], x).astype(BF16)
    for t in range(rows // TILE):
        for i in range(HEADS // 2):
            k_ref[t, i] = k[t * TILE : (t + 1) * TILE, i * double : (i + 1) * double]
        for h in range(HEADS):
            vt_ref[t, h] = v[h * double // 2 : (h + 1) * double // 2, t * TILE : (t + 1) * TILE]
    k = k.astype(F32)
    norms = jnp.dot((k * k).astype(BF16), pick, preferred_element_type=F32)
    norm_ref[0] = norms.reshape(rows // 8, 8, TILE).max(0)


def project(mine, other, w_key, w_value_t, so_far, at, steps):
    width = w_key.shape[0]
    size = width // HEADS
    tiles = 2 * mine.shape[0] // TILE
    return pl.pallas_call(
        project_kernel,
        grid=(1,),
        out_shape=(
            jax.ShapeDtypeStruct((steps * tiles, HEADS // 2, TILE, 2 * size), BF16),
            jax.ShapeDtypeStruct((steps * tiles, HEADS, size, TILE), BF16),
            jax.ShapeDtypeStruct((steps, 8, TILE), F32),
        ),
        in_specs=[vmem()] * 4 + [pl.BlockSpec(memory_space=pl.ANY)] * len(so_far),
        out_specs=(
            pl.BlockSpec((tiles, HEADS // 2, TILE, 2 * size), lambda i: (at, 0, 0, 0)),
            pl.BlockSpec((tiles, HEADS, size, TILE), lambda i: (at, 0, 0, 0)),
            pl.BlockSpec((1, 8, TILE), lambda i: (at, 0, 0)),
        ),
        input_output_aliases={4 + i: i for i in range(len(so_far))},
        compiler_params=pltpu.CompilerParams(vmem_limit_bytes=LIMIT),
        name="project",
    )(mine, other, w_key, w_value_t, *so_far)


def split3(x):
    hi = x.astype(BF16)
    rest = x - hi.astype(F32)
    mid = rest.astype(BF16)
    low = (rest - mid.astype(F32)).astype(BF16)
    return [hi, mid, low]


def attend_kernel(
    index_ref, mine_ref, other_ref, f_ref, wqt_ref, k_ref, vt_ref, norm_ref, out_ref, q_ref, mask_ref,
    acc_ref, max_ref, list_ref, *, chunk, sinks
):
    tiles, _, _, double = k_ref.shape
    size = double // 2
    width = HEADS * size
    nodes = f_ref.shape[0]
    factor = LOG2E / math.sqrt(size)

    start = chunk * (nodes // TILE) * tiles

    def gather(n, found):
        list_ref[found] = n
        used = index_ref[start + n] >= 0
        for t in range(1, nodes // TILE):
            used = used | (index_ref[start + t * tiles + n] >= 0)
        return found + jnp.where(used, 1, 0)

    found = lax.fori_loop(0, tiles, gather, 0)
    groups = (found + GROUP - 1) // GROUP
    bit = lax.shift_left(jnp.int32(1), lax.broadcasted_iota(jnp.int32, (32, TILE), 0))

    def mask(i, carry):
        live = i < found
        n = jnp.where(live, list_ref[i], 0)
        list_ref[i] = n
        for t in range(nodes // TILE):
            e = index_ref[start + t * tiles + n]
            at = jnp.maximum(e, 0)
            words = jnp.where(n // 2 % 2 == 0, mine_ref[at], other_ref[at])
            words = jnp.where(live & (e >= 0), words, 0)
            for w in range(4):
                row = jnp.broadcast_to(words[w : w + 1, :], (32, TILE))
                mask_ref[i, w * 32 : (w + 1) * 32, t * TILE : (t + 1) * TILE] = jnp.where(
                    (row & bit) != 0, F32(1), F32(0)
                ).astype(BF16)
        return carry

    lax.fori_loop(0, groups * GROUP, mask, 0)

    q = nt_dot(wqt_ref[...], f_ref[...]).astype(BF16)
    lower = lax.broadcasted_iota(jnp.int32, (double, nodes), 0) < size
    first = lax.broadcasted_iota(jnp.int32, (size + 16, nodes), 0) == size
    longest = norm_ref[...].max(0).max(0, keepdims=True).max(1, keepdims=True)
    bounds = []
    for h in range(HEADS):
        pair = q[(h // 2) * double : (h // 2 + 1) * double, :]
        q_ref[h // 2, 0:double, h % 2 * nodes : (h % 2 + 1) * nodes] = jnp.where(lower == (h % 2 == 0), pair, jnp.zeros_like(pair))
        mine = q[h * size : (h + 1) * size, :].astype(F32)
        bounds.append(jnp.sqrt((mine * mine).sum(0, keepdims=True) * longest) * F32(1.02))
    bound = jnp.concatenate(bounds, axis=0)
    calm = jnp.max(bound) * F32(factor) <= F32(80)

    @pl.when(calm)
    def _():
        sink = jnp.exp2(bound * -factor) * F32(sinks)
        pieces = [jnp.zeros_like(x) - x for x in split3(bound)]
        for h in range(HEADS):
            column = jnp.concatenate(
                [x[h : h + 1, :].astype(F32) for x in pieces] + [jnp.zeros((13, nodes), F32)], axis=0
            )
            q_ref[h // 2, double : double + 16, h % 2 * nodes : (h % 2 + 1) * nodes] = column.astype(BF16)
            q_ref[h // 2, double + 16 : 2 * double, h % 2 * nodes : (h % 2 + 1) * nodes] = jnp.zeros((double - 16, nodes), BF16)
            max_ref[h] = bound[h : h + 1, :] * F32(factor)
            acc_ref[h] = jnp.where(first, sink[h : h + 1, :], F32(0))
        ones = jnp.ones((16, TILE * GROUP), BF16)
        lane = lax.broadcasted_iota(jnp.int32, (TILE, double), 1)
        units = jnp.where(lane < 3, F32(1), F32(0)).astype(BF16)

        def step(i, carry):
            picked = [list_ref[i * GROUP + g] for g in range(GROUP)]
            keep = jnp.concatenate([mask_ref[i * GROUP + g] for g in range(GROUP)], axis=0)
            keep = jnp.concatenate([keep, keep], axis=1)

            def scores(m):
                keys = [jnp.concatenate([k_ref[n, m], units], axis=1) for n in picked]
                return jnp.dot(jnp.concatenate(keys, axis=0), q_ref[m], preferred_element_type=F32)

            ahead = scores(0)
            for m in range(HEADS // 2):
                s = ahead
                if m + 1 < HEADS // 2:
                    ahead = scores(m + 1)
                p = jnp.exp2(s * F32(factor)).astype(BF16) * keep
                for o in range(2):
                    h = 2 * m + o
                    values = jnp.concatenate([vt_ref[n, h] for n in picked], axis=1)
                    values = jnp.concatenate([values, ones], axis=0)
                    acc_ref[h] = acc_ref[h] + jnp.dot(
                        values, p[:, o * nodes : (o + 1) * nodes], preferred_element_type=F32
                    )
            return carry

        lax.fori_loop(0, groups, step, 0)

    @pl.when(jnp.logical_not(calm))
    def _():
        for h in range(HEADS):
            max_ref[h] = jnp.zeros((1, nodes), F32)
            acc_ref[h] = jnp.where(first, F32(sinks), F32(0))
        ones = jnp.ones((16, TILE), BF16)

        def step(i, carry):
            n = list_ref[i]

            def pair(m, carry):
                both = jnp.dot(k_ref[n, m], q_ref[m, 0:double, :], preferred_element_type=F32)
                for o in range(2):
                    h = 2 * m + o
                    s = both[:, o * nodes : (o + 1) * nodes] * F32(factor)
                    s = jnp.where(mask_ref[i].astype(F32) > 0, s, F32(-jnp.inf))
                    old = max_ref[h]
                    top = jnp.maximum(old, s.max(0, keepdims=True))
                    max_ref[h] = top
                    p = jnp.exp2(s - top).astype(BF16)
                    values = jnp.concatenate([vt_ref[n, h], ones], axis=0)
                    acc_ref[h] = acc_ref[h] * jnp.exp2(old - top) + jnp.dot(
                        values, p, preferred_element_type=F32
                    )
                return carry

            return lax.fori_loop(0, HEADS // 2, pair, carry)

        lax.fori_loop(0, found, step, 0)

    tops, dens = [], []
    for h in range(HEADS):
        den = acc_ref[h, size : size + 1, :]
        out_ref[h * size : (h + 1) * size, :] = (acc_ref[h, 0:size, :] / den).astype(BF16)
        tops.append(max_ref[h])
        dens.append(den)
    stats = split3(jnp.concatenate(tops + dens, axis=0))
    for i, part in enumerate(stats):
        out_ref[width + i * 16 : width + (i + 1) * 16, :] = part


def attend(table, mine, other, feats, w_query_t, keys, values_t, norms, chunk, sinks):
    nodes, width = feats.shape
    size = width // HEADS
    room = (keys.shape[0] + GROUP - 1) // GROUP * GROUP
    return pl.pallas_call(
        functools.partial(attend_kernel, chunk=chunk, sinks=sinks),
        out_shape=jax.ShapeDtypeStruct((width + 48, nodes), BF16),
        in_specs=[smem()] + [vmem()] * 7,
        out_specs=vmem(),
        scratch_shapes=[
            VMEM((HEADS // 2, 4 * size, 2 * nodes), BF16),
            VMEM((room, TILE, nodes), BF16),
            VMEM((HEADS, size + 16, nodes), F32),
            VMEM((HEADS, 1, nodes), F32),
            SMEM((room + 1,), jnp.int32),
        ],
        compiler_params=pltpu.CompilerParams(vmem_limit_bytes=LIMIT),
        name="attend",
    )(table, mine, other, feats, w_query_t, keys, values_t, norms)


def finish_kernel(*refs):
    parts, (w_ref, out_ref) = refs[:-2], refs[-2:]
    width = w_ref.shape[0]
    size = width // HEADS
    tops, dens = [], []
    for part in parts:
        stats = (
            part[width : width + 16, :].astype(F32)
            + part[width + 16 : width + 32, :].astype(F32)
            + part[width + 32 : width + 48, :].astype(F32)
        )
        tops.append(stats[0:HEADS])
        dens.append(stats[HEADS : 2 * HEADS])
    top = functools.reduce(jnp.maximum, tops)
    weights = [jnp.exp2(t - top) * d for t, d in zip(tops, dens)]
    total = functools.reduce(jnp.add, weights)
    rows = []
    for h in range(HEADS):
        num = functools.reduce(
            jnp.add,
            [
                part[h * size : (h + 1) * size, :].astype(F32) * weight[h : h + 1, :]
                for part, weight in zip(parts, weights)
            ],
        )
        rows.append((num / total[h : h + 1, :]).astype(BF16))
    attended = jnp.concatenate(rows, axis=0)
    out_ref[...] = lax.dot_general(
        attended, w_ref[...], (((0,), (0,)), ((), ())), preferred_element_type=F32
    ).astype(BF16)


def finish(parts, w_out):
    nodes = parts[0].shape[1]
    return pl.pallas_call(
        finish_kernel,
        out_shape=jax.ShapeDtypeStruct((nodes, w_out.shape[1]), BF16),
        in_specs=[vmem()] * (len(parts) + 1),
        out_specs=vmem(),
        name="finish",
    )(*parts, w_out)


def body(features, w_query, w_key, w_value, w_out, pairs, counts, masks):
    nrow, ncol = lax.axis_size("row"), lax.axis_size("col")
    nodes, _ = features.shape
    per = nodes // TILE
    row, col = lax.axis_index("row"), lax.axis_index("col")
    chips = ncol // 2
    tiles = 2 * nrow * per
    entries = pairs.shape[2]

    asking = [features] + [None] * (chips - 1)
    near = [features] + [None] * (nrow - 1)
    far = list(range(chips // 2, chips)) + list(range(1, chips // 2))
    for s in range(1, nrow):
        near[s] = exchange(features, "row", s)
    for s in far:
        asking[s] = exchange(features, "col", 2 * s)
    mine = jnp.swapaxes(masks[0, 0], 1, 2)
    other = exchange(mine, "col", 1)
    listed = jnp.concatenate([pairs.reshape(-1), counts.reshape(-1)])
    theirs = exchange(listed, "col", 1)
    table = index(listed, theirs, row, col, chips * per * tiles, tiles, entries)

    w_value_t, w_query_t = w_value.T, w_query.T
    ready = ()
    for s in range(nrow):
        twin = exchange(near[s], "col", 1)
        ready = project(near[s], twin, w_key, w_value_t, ready, s, nrow)

    parts = [None] * chips
    for s in far + [0]:
        part = attend(table, mine, other, asking[s], w_query_t, *ready, s, 2)
        parts[s] = part if s == 0 else exchange(part, "col", 2 * s)
    return finish(parts, w_out)


def solution(mesh):
    in_specs = (
        P(("row", "col"), None),
        P(),
        P(),
        P(),
        P(),
        P("row", "col", None, None),
        P("row", "col"),
        P("row", "col", None, None, None),
    )
    out_specs = P(("row", "col"), None)

    return jax.shard_map(body, mesh=mesh, in_specs=in_specs, out_specs=out_specs, check_vma=False)
```

```python
import functools
import math

import jax
import jax.numpy as jnp
from jax import lax
from jax.experimental import pallas as pl
from jax.experimental.pallas import tpu as pltpu
from jax.sharding import PartitionSpec as P


HEADS = 8
TILE = 128
GROUP = 4
LIMIT = 24 * 1024 * 1024
VMEM = pltpu.VMEM
SMEM = pltpu.SMEM
BF16 = jnp.bfloat16
F32 = jnp.float32
LOG2E = math.log2(math.e)


def vmem():
    return pl.BlockSpec(memory_space=VMEM)


def smem():
    return pl.BlockSpec(memory_space=SMEM)


def exchange(x, axis, bits):
    size = lax.axis_size(axis)
    return lax.ppermute(x, axis, [(i, i ^ bits) for i in range(size)])


def index_kernel(mine_ref, count_ref, other_ref, other_count_ref, out_ref, *, tiles):
    row, col = lax.axis_index("row"), lax.axis_index("col")
    entries = mine_ref.shape[1]
    order = lax.broadcasted_iota(jnp.int32, (1, entries), 1)
    number = lax.broadcasted_iota(jnp.int32, (entries, TILE), 0) + 1
    lane = lax.broadcasted_iota(jnp.int32, (entries, TILE), 1)
    spots = []
    for side, (ref, count) in enumerate(((mine_ref, count_ref), (other_ref, other_count_ref))):
        a, b = ref[0:1, :], ref[1:2, :]
        chunk = (a >> 1) ^ col
        tile = (((b >> 1) ^ row) << 2) + side * 2 + (b & 1)
        good = (order < count[0, 0]) & ((chunk & 1) == 0)
        spot = jnp.where(good, (chunk + (a & 1)) * tiles + tile, -1)
        spots.append(jnp.broadcast_to(spot.astype(F32), (TILE, entries)).T.astype(jnp.int32))
    for block in range(out_ref.shape[1] // TILE):
        found = jnp.zeros((1, TILE), jnp.int32)
        for spot in spots:
            here = jnp.where(spot == lane + block * TILE, number, 0)
            found = found + here.sum(0, keepdims=True)
        out_ref[0:1, block * TILE : (block + 1) * TILE] = found - 1


def cost(microseconds):
    return pl.CostEstimate(flops=int(microseconds * 9e8), bytes_accessed=0, transcendentals=0)


def index(mine, count, other, other_count, size, tiles):
    return pl.pallas_call(
        functools.partial(index_kernel, tiles=tiles),
        out_shape=jax.ShapeDtypeStruct((1, (size + TILE - 1) // TILE * TILE), jnp.int32),
        in_specs=[vmem(), smem(), vmem(), smem()],
        out_specs=vmem(),
        cost_estimate=cost(3),
        compiler_params=pltpu.CompilerParams(vmem_limit_bytes=LIMIT),
        name="index",
    )(mine, count, other, other_count)


def turn_kernel(after_ref, a_ref, b_ref, at_ref, bt_ref):
    at_ref[...] = a_ref[...].T
    bt_ref[...] = b_ref[...].T


def turn(after, a, b):
    return pl.pallas_call(
        turn_kernel,
        out_shape=tuple(jax.ShapeDtypeStruct(x.shape[::-1], BF16) for x in (a, b)),
        in_specs=[vmem()] * 3,
        out_specs=(vmem(),) * 2,
        cost_estimate=cost(1),
        compiler_params=pltpu.CompilerParams(vmem_limit_bytes=LIMIT),
        name="turn",
    )(after, a, b)


def nt_dot(a, b):
    return lax.dot_general(a, b, (((1,), (1,)), ((), ())), preferred_element_type=F32)


def project_kernel(mine_ref, other_ref, wk_ref, wvt_ref, *refs):
    k_ref, vt_ref, norm_ref = refs[-3:]
    double = k_ref.shape[3]
    width = wk_ref.shape[0]
    lane = lax.broadcasted_iota(jnp.int32, (width, TILE), 1)
    head = lax.broadcasted_iota(jnp.int32, (width, TILE), 0) // (double // 2)
    pick = jnp.where(lane == head, F32(1.01), F32(0)).astype(BF16)
    x = jnp.concatenate([mine_ref[...], other_ref[...]], axis=0)
    rows = x.shape[0]
    k = jnp.dot(x, wk_ref[...], preferred_element_type=F32).astype(BF16)
    v = nt_dot(wvt_ref[...], x).astype(BF16)
    for t in range(rows // TILE):
        for i in range(HEADS // 2):
            k_ref[t, i] = k[t * TILE : (t + 1) * TILE, i * double : (i + 1) * double]
        for h in range(HEADS):
            vt_ref[t, h] = v[h * double // 2 : (h + 1) * double // 2, t * TILE : (t + 1) * TILE]
    k = k.astype(F32)
    norms = jnp.dot((k * k).astype(BF16), pick, preferred_element_type=F32)
    norm_ref[0] = norms.reshape(rows // 8, 8, TILE).max(0)


def project(mine, other, w_key, w_value_t, so_far, at, steps):
    width = w_key.shape[0]
    size = width // HEADS
    tiles = 2 * mine.shape[0] // TILE
    return pl.pallas_call(
        project_kernel,
        grid=(1,),
        out_shape=(
            jax.ShapeDtypeStruct((steps * tiles, HEADS // 2, TILE, 2 * size), BF16),
            jax.ShapeDtypeStruct((steps * tiles, HEADS, size, TILE), BF16),
            jax.ShapeDtypeStruct((steps, 8, TILE), F32),
        ),
        in_specs=[vmem()] * 4 + [pl.BlockSpec(memory_space=pl.ANY)] * len(so_far),
        out_specs=(
            pl.BlockSpec((tiles, HEADS // 2, TILE, 2 * size), lambda i: (at, 0, 0, 0)),
            pl.BlockSpec((tiles, HEADS, size, TILE), lambda i: (at, 0, 0, 0)),
            pl.BlockSpec((1, 8, TILE), lambda i: (at, 0, 0)),
        ),
        input_output_aliases={4 + i: i for i in range(len(so_far))},
        cost_estimate=cost(1),
        compiler_params=pltpu.CompilerParams(vmem_limit_bytes=LIMIT),
        name="project",
    )(mine, other, w_key, w_value_t, *so_far)


def split3(x):
    hi = x.astype(BF16)
    rest = x - hi.astype(F32)
    mid = rest.astype(BF16)
    low = (rest - mid.astype(F32)).astype(BF16)
    return [hi, mid, low]


def attend_kernel(
    index_ref, mine_ref, other_ref, f_ref, wqt_ref, k_ref, vt_ref, norm_ref, out_ref, q_ref, mask_ref,
    acc_ref, max_ref, list_ref, *, chunk, sinks
):
    tiles, _, _, double = k_ref.shape
    size = double // 2
    width = HEADS * size
    nodes = f_ref.shape[0]
    factor = LOG2E / math.sqrt(size)

    start = chunk * (nodes // TILE) * tiles

    def gather(n, found):
        list_ref[found] = n
        used = index_ref[0, start + n] >= 0
        for t in range(1, nodes // TILE):
            used = used | (index_ref[0, start + t * tiles + n] >= 0)
        return found + jnp.where(used, 1, 0)

    found = lax.fori_loop(0, tiles, gather, 0)
    groups = (found + GROUP - 1) // GROUP
    bit = lax.shift_left(jnp.int32(1), lax.broadcasted_iota(jnp.int32, (32, TILE), 0))

    def mask(i, carry):
        live = i < found
        n = jnp.where(live, list_ref[i], 0)
        list_ref[i] = n
        for t in range(nodes // TILE):
            e = index_ref[0, start + t * tiles + n]
            at = jnp.maximum(e, 0)
            words = jnp.where(n // 2 % 2 == 0, mine_ref[at], other_ref[at])
            words = jnp.where(live & (e >= 0), words, 0)
            for w in range(4):
                row = jnp.broadcast_to(words[w : w + 1, :], (32, TILE))
                mask_ref[i, w * 32 : (w + 1) * 32, t * TILE : (t + 1) * TILE] = jnp.where(
                    (row & bit) != 0, F32(1), F32(0)
                ).astype(BF16)
        return carry

    lax.fori_loop(0, groups * GROUP, mask, 0)

    q = nt_dot(wqt_ref[...], f_ref[...]).astype(BF16)
    lower = lax.broadcasted_iota(jnp.int32, (double, nodes), 0) < size
    first = lax.broadcasted_iota(jnp.int32, (size + 16, nodes), 0) == size
    longest = norm_ref[...].max(0).max(0, keepdims=True).max(1, keepdims=True)
    bounds = []
    for h in range(HEADS):
        pair = q[(h // 2) * double : (h // 2 + 1) * double, :]
        q_ref[h // 2, 0:double, h % 2 * nodes : (h % 2 + 1) * nodes] = jnp.where(lower == (h % 2 == 0), pair, jnp.zeros_like(pair))
        mine = q[h * size : (h + 1) * size, :].astype(F32)
        bounds.append(jnp.sqrt((mine * mine).sum(0, keepdims=True) * longest) * F32(1.02))
    bound = jnp.concatenate(bounds, axis=0)
    calm = jnp.max(bound) * F32(factor) <= F32(80)

    @pl.when(calm)
    def _():
        sink = jnp.exp2(bound * -factor) * F32(sinks)
        pieces = [jnp.zeros_like(x) - x for x in split3(bound)]
        for h in range(HEADS):
            column = jnp.concatenate(
                [x[h : h + 1, :].astype(F32) for x in pieces] + [jnp.zeros((13, nodes), F32)], axis=0
            )
            q_ref[h // 2, double : double + 16, h % 2 * nodes : (h % 2 + 1) * nodes] = column.astype(BF16)
            q_ref[h // 2, double + 16 : 2 * double, h % 2 * nodes : (h % 2 + 1) * nodes] = jnp.zeros((double - 16, nodes), BF16)
            max_ref[h] = bound[h : h + 1, :] * F32(factor)
            acc_ref[h] = jnp.where(first, sink[h : h + 1, :], F32(0))
        ones = jnp.ones((16, TILE * GROUP), BF16)
        lane = lax.broadcasted_iota(jnp.int32, (TILE, double), 1)
        units = jnp.where(lane < 3, F32(1), F32(0)).astype(BF16)

        def step(i, carry):
            picked = [list_ref[i * GROUP + g] for g in range(GROUP)]
            keep = jnp.concatenate([mask_ref[i * GROUP + g] for g in range(GROUP)], axis=0)
            keep = jnp.concatenate([keep, keep], axis=1)

            def scores(m):
                keys = [jnp.concatenate([k_ref[n, m], units], axis=1) for n in picked]
                return jnp.dot(jnp.concatenate(keys, axis=0), q_ref[m], preferred_element_type=F32)

            ahead = scores(0)
            for m in range(HEADS // 2):
                s = ahead
                if m + 1 < HEADS // 2:
                    ahead = scores(m + 1)
                p = jnp.exp2(s * F32(factor)).astype(BF16) * keep
                for o in range(2):
                    h = 2 * m + o
                    values = jnp.concatenate([vt_ref[n, h] for n in picked], axis=1)
                    values = jnp.concatenate([values, ones], axis=0)
                    acc_ref[h] = acc_ref[h] + jnp.dot(
                        values, p[:, o * nodes : (o + 1) * nodes], preferred_element_type=F32
                    )
            return carry

        lax.fori_loop(0, groups, step, 0)

    @pl.when(jnp.logical_not(calm))
    def _():
        for h in range(HEADS):
            max_ref[h] = jnp.zeros((1, nodes), F32)
            acc_ref[h] = jnp.where(first, F32(sinks), F32(0))
        ones = jnp.ones((16, TILE), BF16)

        def step(i, carry):
            n = list_ref[i]

            def pair(m, carry):
                both = jnp.dot(k_ref[n, m], q_ref[m, 0:double, :], preferred_element_type=F32)
                for o in range(2):
                    h = 2 * m + o
                    s = both[:, o * nodes : (o + 1) * nodes] * F32(factor)
                    s = jnp.where(mask_ref[i].astype(F32) > 0, s, F32(-jnp.inf))
                    old = max_ref[h]
                    top = jnp.maximum(old, s.max(0, keepdims=True))
                    max_ref[h] = top
                    p = jnp.exp2(s - top).astype(BF16)
                    values = jnp.concatenate([vt_ref[n, h], ones], axis=0)
                    acc_ref[h] = acc_ref[h] * jnp.exp2(old - top) + jnp.dot(
                        values, p, preferred_element_type=F32
                    )
                return carry

            return lax.fori_loop(0, HEADS // 2, pair, carry)

        lax.fori_loop(0, found, step, 0)

    tops, dens = [], []
    for h in range(HEADS):
        den = acc_ref[h, size : size + 1, :]
        out_ref[h * size : (h + 1) * size, :] = (acc_ref[h, 0:size, :] / den).astype(BF16)
        tops.append(max_ref[h])
        dens.append(den)
    stats = split3(jnp.concatenate(tops + dens, axis=0))
    for i, part in enumerate(stats):
        out_ref[width + i * 16 : width + (i + 1) * 16, :] = part


def attend(table, mine, other, feats, w_query_t, keys, values_t, norms, chunk, sinks):
    nodes, width = feats.shape
    size = width // HEADS
    room = (keys.shape[0] + GROUP - 1) // GROUP * GROUP
    return pl.pallas_call(
        functools.partial(attend_kernel, chunk=chunk, sinks=sinks),
        out_shape=jax.ShapeDtypeStruct((width + 48, nodes), BF16),
        in_specs=[smem()] + [vmem()] * 7,
        out_specs=vmem(),
        scratch_shapes=[
            VMEM((HEADS // 2, 4 * size, 2 * nodes), BF16),
            VMEM((room, TILE, nodes), BF16),
            VMEM((HEADS, size + 16, nodes), F32),
            VMEM((HEADS, 1, nodes), F32),
            SMEM((room + 1,), jnp.int32),
        ],
        cost_estimate=cost(4),
        compiler_params=pltpu.CompilerParams(vmem_limit_bytes=LIMIT),
        name="attend",
    )(table, mine, other, feats, w_query_t, keys, values_t, norms)


def finish_kernel(*refs):
    count = (len(refs) - 4) // 2
    own, far, (w_ref, out_ref) = refs[0], refs[1 : count + 1], refs[count + 1 : count + 3]
    near, sems = refs[count + 3 : -1], refs[-1]
    copies = [pltpu.make_async_copy(a, b, sems.at[i]) for i, (a, b) in enumerate(zip(far, near))]
    for copy in copies:
        copy.start()
    for copy in copies:
        copy.wait()
    parts = [own] + list(near)
    width = w_ref.shape[0]
    size = width // HEADS
    tops, dens = [], []
    for part in parts:
        stats = (
            part[width : width + 16, :].astype(F32)
            + part[width + 16 : width + 32, :].astype(F32)
            + part[width + 32 : width + 48, :].astype(F32)
        )
        tops.append(stats[0:HEADS])
        dens.append(stats[HEADS : 2 * HEADS])
    top = functools.reduce(jnp.maximum, tops)
    weights = [jnp.exp2(t - top) * d for t, d in zip(tops, dens)]
    total = functools.reduce(jnp.add, weights)
    rows = []
    for h in range(HEADS):
        num = functools.reduce(
            jnp.add,
            [
                part[h * size : (h + 1) * size, :].astype(F32) * weight[h : h + 1, :]
                for part, weight in zip(parts, weights)
            ],
        )
        rows.append((num / total[h : h + 1, :]).astype(BF16))
    attended = jnp.concatenate(rows, axis=0)
    out_ref[...] = lax.dot_general(
        attended, w_ref[...], (((0,), (0,)), ((), ())), preferred_element_type=F32
    ).astype(BF16)


def finish(parts, w_out):
    nodes = parts[0].shape[1]
    others = len(parts) - 1
    return pl.pallas_call(
        finish_kernel,
        out_shape=jax.ShapeDtypeStruct((nodes, w_out.shape[1]), BF16),
        in_specs=[vmem()] + [pl.BlockSpec(memory_space=pl.ANY)] * others + [vmem()],
        out_specs=vmem(),
        scratch_shapes=[VMEM(parts[0].shape, BF16)] * others + [pltpu.SemaphoreType.DMA((others,))],
        compiler_params=pltpu.CompilerParams(vmem_limit_bytes=LIMIT),
        name="finish",
    )(*parts, w_out)


def body(features, w_query, w_key, w_value, w_out, pairs, counts, masks):
    nrow, ncol = lax.axis_size("row"), lax.axis_size("col")
    nodes, _ = features.shape
    per = nodes // TILE
    chips = ncol // 2
    tiles = 2 * nrow * per

    asking = [features] + [None] * (chips - 1)
    near = [features] + [None] * (nrow - 1)
    half = chips // 2
    asking[half] = exchange(features, "col", 2 * half)
    for s in range(nrow - 1, 0, -1):
        near[s] = exchange(features, "row", s)
    for s in range(1, half):
        asking[s] = exchange(features, "col", 2 * s)
        asking[s + half] = exchange(asking[half], "col", 2 * s)
    mine = jnp.swapaxes(masks[0, 0], 1, 2)
    other = exchange(mine, "col", 1)
    listed = jnp.swapaxes(pairs[0, 0], 0, 1)
    other_listed = exchange(listed, "col", 1)
    other_counts = exchange(counts, "col", 1)
    table = index(listed, counts, other_listed, other_counts, chips * per * tiles, tiles)
    w_query_t, w_value_t = turn(table, w_query, w_value)

    ready = ()
    for s in range(nrow):
        twin = exchange(near[s], "col", 1)
        ready = project(near[s], twin, w_key, w_value_t, ready, s, nrow)

    far = list(range(half, chips)) + list(range(1, half))
    parts = [None] * chips
    for s in far + [0]:
        part = attend(table, mine, other, asking[s], w_query_t, *ready, s, 2)
        parts[s] = part if s == 0 else exchange(part, "col", 2 * s)
    return finish(parts, w_out)


def solution(mesh):
    in_specs = (
        P(("row", "col"), None),
        P(),
        P(),
        P(),
        P(),
        P("row", "col", None, None),
        P("row", "col"),
        P("row", "col", None, None, None),
    )
    out_specs = P(("row", "col"), None)

    return jax.shard_map(body, mesh=mesh, in_specs=in_specs, out_specs=out_specs, check_vma=False)
```

```python
import functools
import math

import jax
import jax.numpy as jnp
from jax import lax
from jax.experimental import pallas as pl
from jax.experimental.pallas import tpu as pltpu
from jax.sharding import PartitionSpec as P


HEADS = 8
TILE = 128
GROUP = 4
LIMIT = 24 * 1024 * 1024
VMEM = pltpu.VMEM
SMEM = pltpu.SMEM
BF16 = jnp.bfloat16
F32 = jnp.float32
LOG2E = math.log2(math.e)


def vmem():
    return pl.BlockSpec(memory_space=VMEM)


def smem():
    return pl.BlockSpec(memory_space=SMEM)


def exchange(x, axis, bits):
    size = lax.axis_size(axis)
    return lax.ppermute(x, axis, [(i, i ^ bits) for i in range(size)])


def index_kernel(mine_ref, count_ref, other_ref, other_count_ref, out_ref, *, tiles):
    row, col = lax.axis_index("row"), lax.axis_index("col")
    entries = mine_ref.shape[1]
    order = lax.broadcasted_iota(jnp.int32, (1, entries), 1)
    number = lax.broadcasted_iota(jnp.int32, (entries, TILE), 0) + 1
    lane = lax.broadcasted_iota(jnp.int32, (entries, TILE), 1)
    spots = []
    for side, (ref, count) in enumerate(((mine_ref, count_ref), (other_ref, other_count_ref))):
        a, b = ref[0:1, :], ref[1:2, :]
        chunk = (a >> 1) ^ col
        tile = (((b >> 1) ^ row) << 2) + side * 2 + (b & 1)
        good = (order < count[0, 0]) & ((chunk & 1) == 0)
        spot = jnp.where(good, (chunk + (a & 1)) * tiles + tile, -1)
        spots.append(jnp.broadcast_to(spot.astype(F32), (TILE, entries)).T.astype(jnp.int32))
    for block in range(out_ref.shape[1] // TILE):
        found = jnp.zeros((1, TILE), jnp.int32)
        for spot in spots:
            here = jnp.where(spot == lane + block * TILE, number, 0)
            found = found + here.sum(0, keepdims=True)
        out_ref[0:1, block * TILE : (block + 1) * TILE] = found - 1


def cost(microseconds):
    return pl.CostEstimate(flops=int(microseconds * 9e8), bytes_accessed=0, transcendentals=0)


def index(mine, count, other, other_count, size, tiles):
    return pl.pallas_call(
        functools.partial(index_kernel, tiles=tiles),
        out_shape=jax.ShapeDtypeStruct((1, (size + TILE - 1) // TILE * TILE), jnp.int32),
        in_specs=[vmem(), smem(), vmem(), smem()],
        out_specs=vmem(),
        cost_estimate=cost(3),
        compiler_params=pltpu.CompilerParams(vmem_limit_bytes=LIMIT),
        name="index",
    )(mine, count, other, other_count)


def turn_kernel(after_ref, a_ref, b_ref, at_ref, bt_ref):
    at_ref[...] = a_ref[...].T
    bt_ref[...] = b_ref[...].T


def turn(after, a, b):
    return pl.pallas_call(
        turn_kernel,
        out_shape=tuple(jax.ShapeDtypeStruct(x.shape[::-1], BF16) for x in (a, b)),
        in_specs=[vmem()] * 3,
        out_specs=(vmem(),) * 2,
        cost_estimate=cost(1),
        compiler_params=pltpu.CompilerParams(vmem_limit_bytes=LIMIT),
        name="turn",
    )(after, a, b)


def nt_dot(a, b):
    return lax.dot_general(a, b, (((1,), (1,)), ((), ())), preferred_element_type=F32)


def project_kernel(mine_ref, other_ref, wk_ref, wvt_ref, *refs):
    k_ref, vt_ref, norm_ref = refs[-3:]
    double = k_ref.shape[3]
    width = wk_ref.shape[0]
    lane = lax.broadcasted_iota(jnp.int32, (width, TILE), 1)
    head = lax.broadcasted_iota(jnp.int32, (width, TILE), 0) // (double // 2)
    pick = jnp.where(lane == head, F32(1.01), F32(0)).astype(BF16)
    x = jnp.concatenate([mine_ref[...], other_ref[...]], axis=0)
    rows = x.shape[0]
    k = jnp.dot(x, wk_ref[...], preferred_element_type=F32).astype(BF16)
    v = nt_dot(wvt_ref[...], x).astype(BF16)
    for t in range(rows // TILE):
        for i in range(HEADS // 2):
            k_ref[t, i] = k[t * TILE : (t + 1) * TILE, i * double : (i + 1) * double]
        for h in range(HEADS):
            vt_ref[t, h] = v[h * double // 2 : (h + 1) * double // 2, t * TILE : (t + 1) * TILE]
    k = k.astype(F32)
    norms = jnp.dot((k * k).astype(BF16), pick, preferred_element_type=F32)
    norm_ref[0] = norms.reshape(rows // 8, 8, TILE).max(0)


def project(mine, other, w_key, w_value_t, so_far, at, steps):
    width = w_key.shape[0]
    size = width // HEADS
    tiles = 2 * mine.shape[0] // TILE
    return pl.pallas_call(
        project_kernel,
        grid=(1,),
        out_shape=(
            jax.ShapeDtypeStruct((steps * tiles, HEADS // 2, TILE, 2 * size), BF16),
            jax.ShapeDtypeStruct((steps * tiles, HEADS, size, TILE), BF16),
            jax.ShapeDtypeStruct((steps, 8, TILE), F32),
        ),
        in_specs=[vmem()] * 4 + [pl.BlockSpec(memory_space=pl.ANY)] * len(so_far),
        out_specs=(
            pl.BlockSpec((tiles, HEADS // 2, TILE, 2 * size), lambda i: (at, 0, 0, 0)),
            pl.BlockSpec((tiles, HEADS, size, TILE), lambda i: (at, 0, 0, 0)),
            pl.BlockSpec((1, 8, TILE), lambda i: (at, 0, 0)),
        ),
        input_output_aliases={4 + i: i for i in range(len(so_far))},
        cost_estimate=cost(1),
        compiler_params=pltpu.CompilerParams(vmem_limit_bytes=LIMIT),
        name="project",
    )(mine, other, w_key, w_value_t, *so_far)


def split3(x):
    hi = x.astype(BF16)
    rest = x - hi.astype(F32)
    mid = rest.astype(BF16)
    low = (rest - mid.astype(F32)).astype(BF16)
    return [hi, mid, low]


def attend_kernel(
    index_ref, mine_ref, other_ref, f_ref, wqt_ref, k_ref, vt_ref, norm_ref, out_ref, q_ref, mask_ref,
    acc_ref, max_ref, list_ref, *, chunk, sinks
):
    tiles, _, _, double = k_ref.shape
    size = double // 2
    width = HEADS * size
    nodes = f_ref.shape[0]
    factor = LOG2E / math.sqrt(size)

    start = chunk * (nodes // TILE) * tiles

    def gather(n, found):
        list_ref[found] = n
        used = index_ref[0, start + n] >= 0
        for t in range(1, nodes // TILE):
            used = used | (index_ref[0, start + t * tiles + n] >= 0)
        return found + jnp.where(used, 1, 0)

    found = lax.fori_loop(0, tiles, gather, 0)
    groups = (found + GROUP - 1) // GROUP
    bit = lax.shift_left(jnp.int32(1), lax.broadcasted_iota(jnp.int32, (32, TILE), 0))

    def mask(group, carry):
        for g in range(GROUP):
            i = group * GROUP + g
            live = i < found
            n = jnp.where(live, list_ref[i], 0)
            list_ref[i] = n
            for t in range(nodes // TILE):
                e = index_ref[0, start + t * tiles + n]
                at = jnp.maximum(e, 0)
                words = jnp.where(n // 2 % 2 == 0, mine_ref[at], other_ref[at])
                words = jnp.where(live & (e >= 0), words, 0)
                for w in range(4):
                    row = jnp.broadcast_to(words[w : w + 1, :], (32, TILE))
                    mask_ref[i, w * 32 : (w + 1) * 32, t * TILE : (t + 1) * TILE] = jnp.where(
                        (row & bit) != 0, F32(1), F32(0)
                    ).astype(BF16)
        return carry

    lax.fori_loop(0, groups, mask, 0)

    q = nt_dot(wqt_ref[...], f_ref[...]).astype(BF16)
    lower = lax.broadcasted_iota(jnp.int32, (double, nodes), 0) < size
    first = lax.broadcasted_iota(jnp.int32, (size + 16, nodes), 0) == size
    longest = norm_ref[...].max(0).max(0, keepdims=True).max(1, keepdims=True)
    bounds = []
    for h in range(HEADS):
        pair = q[(h // 2) * double : (h // 2 + 1) * double, :]
        q_ref[h // 2, 0:double, h % 2 * nodes : (h % 2 + 1) * nodes] = jnp.where(lower == (h % 2 == 0), pair, jnp.zeros_like(pair))
        mine = q[h * size : (h + 1) * size, :].astype(F32)
        bounds.append(jnp.sqrt((mine * mine).sum(0, keepdims=True) * longest) * F32(1.02))
    bound = jnp.concatenate(bounds, axis=0)
    calm = jnp.max(bound) * F32(factor) <= F32(80)

    @pl.when(calm)
    def _():
        sink = jnp.exp2(bound * -factor) * F32(sinks)
        for h in range(HEADS):
            max_ref[h] = bound[h : h + 1, :] * F32(factor)
            acc_ref[h] = jnp.where(first, sink[h : h + 1, :], F32(0))
        ones = jnp.ones((16, TILE * GROUP), BF16)

        def step(i, carry):
            picked = [list_ref[i * GROUP + g] for g in range(GROUP)]
            keep = jnp.concatenate([mask_ref[i * GROUP + g] for g in range(GROUP)], axis=0)
            keep = jnp.concatenate([keep, keep], axis=1)

            def scores(m):
                keys = [k_ref[n, m] for n in picked]
                return jnp.dot(jnp.concatenate(keys, axis=0), q_ref[m], preferred_element_type=F32)

            ahead = scores(0)
            for m in range(HEADS // 2):
                s = ahead
                if m + 1 < HEADS // 2:
                    ahead = scores(m + 1)
                level = jnp.concatenate([max_ref[2 * m], max_ref[2 * m + 1]], axis=1)
                p = jnp.exp2(s * F32(factor) - level).astype(BF16) * keep
                for o in range(2):
                    h = 2 * m + o
                    values = jnp.concatenate([vt_ref[n, h] for n in picked], axis=1)
                    values = jnp.concatenate([values, ones], axis=0)
                    acc_ref[h] = acc_ref[h] + jnp.dot(
                        values, p[:, o * nodes : (o + 1) * nodes], preferred_element_type=F32
                    )
            return carry

        lax.fori_loop(0, groups, step, 0)

    @pl.when(jnp.logical_not(calm))
    def _():
        for h in range(HEADS):
            max_ref[h] = jnp.zeros((1, nodes), F32)
            acc_ref[h] = jnp.where(first, F32(sinks), F32(0))
        ones = jnp.ones((16, TILE), BF16)

        def step(i, carry):
            n = list_ref[i]

            def pair(m, carry):
                both = jnp.dot(k_ref[n, m], q_ref[m, 0:double, :], preferred_element_type=F32)
                for o in range(2):
                    h = 2 * m + o
                    s = both[:, o * nodes : (o + 1) * nodes] * F32(factor)
                    s = jnp.where(mask_ref[i].astype(F32) > 0, s, F32(-jnp.inf))
                    old = max_ref[h]
                    top = jnp.maximum(old, s.max(0, keepdims=True))
                    max_ref[h] = top
                    p = jnp.exp2(s - top).astype(BF16)
                    values = jnp.concatenate([vt_ref[n, h], ones], axis=0)
                    acc_ref[h] = acc_ref[h] * jnp.exp2(old - top) + jnp.dot(
                        values, p, preferred_element_type=F32
                    )
                return carry

            return lax.fori_loop(0, HEADS // 2, pair, carry)

        lax.fori_loop(0, found, step, 0)

    tops, dens = [], []
    for h in range(HEADS):
        den = acc_ref[h, size : size + 1, :]
        out_ref[h * size : (h + 1) * size, :] = (acc_ref[h, 0:size, :] / den).astype(BF16)
        tops.append(max_ref[h])
        dens.append(den)
    pieces = split3(jnp.concatenate(tops, axis=0)) + split3(jnp.concatenate(dens, axis=0))[:2]
    out_ref[width : width + 5 * HEADS, :] = jnp.concatenate([x.astype(F32) for x in pieces], axis=0).astype(BF16)


def attend(table, mine, other, feats, w_query_t, keys, values_t, norms, chunk, sinks):
    nodes, width = feats.shape
    size = width // HEADS
    room = (keys.shape[0] + GROUP - 1) // GROUP * GROUP
    return pl.pallas_call(
        functools.partial(attend_kernel, chunk=chunk, sinks=sinks),
        out_shape=jax.ShapeDtypeStruct((width + 5 * HEADS, nodes), BF16),
        in_specs=[smem()] + [vmem()] * 7,
        out_specs=vmem(),
        scratch_shapes=[
            VMEM((HEADS // 2, 2 * size, 2 * nodes), BF16),
            VMEM((room, TILE, nodes), BF16),
            VMEM((HEADS, size + 16, nodes), F32),
            VMEM((HEADS, 1, nodes), F32),
            SMEM((room + 1,), jnp.int32),
        ],
        cost_estimate=cost(4),
        compiler_params=pltpu.CompilerParams(vmem_limit_bytes=LIMIT),
        name="attend",
    )(table, mine, other, feats, w_query_t, keys, values_t, norms)


def finish_kernel(*refs):
    parts, (w_ref, out_ref) = refs[:-2], refs[-2:]
    width = w_ref.shape[0]
    size = width // HEADS
    tops, dens = [], []
    for part in parts:
        stats = part[width : width + 5 * HEADS, :].astype(F32)
        pieces = [stats[i * HEADS : (i + 1) * HEADS] for i in range(5)]
        tops.append(pieces[0] + pieces[1] + pieces[2])
        dens.append(pieces[3] + pieces[4])
    top = functools.reduce(jnp.maximum, tops)
    weights = [jnp.exp2(t - top) * d for t, d in zip(tops, dens)]
    total = functools.reduce(jnp.add, weights)
    rows = []
    for h in range(HEADS):
        num = functools.reduce(
            jnp.add,
            [
                part[h * size : (h + 1) * size, :].astype(F32) * weight[h : h + 1, :]
                for part, weight in zip(parts, weights)
            ],
        )
        rows.append((num / total[h : h + 1, :]).astype(BF16))
    attended = jnp.concatenate(rows, axis=0)
    out_ref[...] = lax.dot_general(
        attended, w_ref[...], (((0,), (0,)), ((), ())), preferred_element_type=F32
    ).astype(BF16)


def finish(parts, w_out):
    nodes = parts[0].shape[1]
    return pl.pallas_call(
        finish_kernel,
        out_shape=jax.ShapeDtypeStruct((nodes, w_out.shape[1]), BF16),
        in_specs=[vmem()] * (len(parts) + 1),
        out_specs=vmem(),
        compiler_params=pltpu.CompilerParams(vmem_limit_bytes=LIMIT),
        name="finish",
    )(*parts, w_out)


def turn_order(chips):
    half = chips // 2
    return list(range(half, chips)) + list(range(1, half))


def body(features, w_query, w_key, w_value, w_out, pairs, counts, masks):
    nrow, ncol = lax.axis_size("row"), lax.axis_size("col")
    nodes, _ = features.shape
    per = nodes // TILE
    chips = ncol // 2
    tiles = 2 * nrow * per

    asking = [features] + [None] * (chips - 1)
    near = [features] + [None] * (nrow - 1)
    half = chips // 2
    asking[half] = exchange(features, "col", 2 * half)
    for s in range(nrow - 1, 0, -1):
        near[s] = exchange(features, "row", s)
    for s in range(1, half):
        asking[s] = exchange(features, "col", 2 * s)
        asking[s + half] = exchange(asking[half], "col", 2 * s)
    mine = jnp.swapaxes(masks[0, 0], 1, 2)
    other = exchange(mine, "col", 1)
    listed = jnp.swapaxes(pairs[0, 0], 0, 1)
    other_listed = exchange(listed, "col", 1)
    other_counts = exchange(counts, "col", 1)
    table = index(listed, counts, other_listed, other_counts, chips * per * tiles, tiles)
    w_query_t, w_value_t = turn(table, w_query, w_value)

    ready = ()
    for s in range(nrow):
        twin = exchange(near[s], "col", 1)
        ready = project(near[s], twin, w_key, w_value_t, ready, s, nrow)

    far = turn_order(chips)
    parts = [None] * chips
    for s in far + [0]:
        part = attend(table, mine, other, asking[s], w_query_t, *ready, s, 2)
        parts[s] = part if s == 0 else exchange(part, "col", 2 * s)
    return finish(parts, w_out)


def solution(mesh):
    in_specs = (
        P(("row", "col"), None),
        P(),
        P(),
        P(),
        P(),
        P("row", "col", None, None),
        P("row", "col"),
        P("row", "col", None, None, None),
    )
    out_specs = P(("row", "col"), None)

    return jax.shard_map(body, mesh=mesh, in_specs=in_specs, out_specs=out_specs, check_vma=False)
```
